32 devices in a mesh: tensor: 4 (over y, x), seq: 8 (over z, core).
Axes of the slice: x: 2, y: 2, z: 4, core: 2. Of those that a mesh axis runs over, the one named last changes fastest.
Arguments:
- key_states: bfloat16 [8, 2, 4096, 1024], P(None, None, 'seq', 'tensor'), may hold values from -6 to 6
- value_states: bfloat16 [8, 2, 4096, 1024], P(None, None, 'seq', 'tensor'), may hold values from -6 to 6
- bin_index: int32 [8, 8, 4096], P(None, 'tensor', 'seq'), may hold values from 0 to 4095
- retain_count: int32 [8], replicated, may hold values from 1 to 4096
Outputs:
- histogram: float32 [8, 8, 2, 4096], P(None, 'tensor', None, 'seq')
- threshold: int32 [8], replicated
The draws below stay inside these ranges and needn't reach their ends.
All inputs are finite; a program needn't handle non-finite values.
Results may differ from the reference program's by a relative error of at most 0.0029.
Values sent between devices are 32-bit elements; how exact they have to be, the bound alone decides.
No kernel may reach another device: no remote copies, remote signals or barrier semaphores. Data moves between devices by JAX's collectives and lax.ppermute only.
A program may use at most 64 MiB of HBM per device.

```python
import jax
import jax.numpy as jnp
from jax import lax

KVH = 8
HD = 128
BINS = 4096
PAIRS = 8
TOK_DEV = 512
TOKENS = 4096


def draw_bin_index(key, part):
    blocks = TOKENS // TOK_DEV
    key_centre = jax.random.fold_in(key, 11)
    key_expo = jax.random.fold_in(key, 12)
    key_first = jax.random.fold_in(key, 13)
    key_second = jax.random.fold_in(key, 14)
    centre = jax.random.randint(key_centre, (PAIRS, KVH, blocks, 1), 0, BINS).astype(jnp.int32)
    expo = jax.random.randint(key_expo, (PAIRS, KVH, blocks, 1), 0, 8).astype(jnp.int32)
    spread = jnp.maximum(BINS // jnp.left_shift(jnp.ones_like(expo), expo), 1)
    first = jax.random.randint(key_first, (PAIRS, KVH, blocks, TOK_DEV), 0, BINS).astype(jnp.int32) % spread
    second = jax.random.randint(key_second, (PAIRS, KVH, blocks, TOK_DEV), 0, BINS).astype(jnp.int32) % spread
    placed = (centre + first + second) % BINS
    return placed.reshape(PAIRS, KVH, TOKENS).astype(jnp.int32)


def draw_retain_count(key, part):
    key_count = jax.random.fold_in(key, 21)
    highest = min(4096, TOKENS * KVH)
    return jax.random.randint(key_count, (PAIRS,), 1, highest + 1).astype(jnp.int32)


def block_scale(stream_key, shape, shards, smallest, largest):
    loudness = 1.0
    for position, blocks in shards:
        heights = jax.random.uniform(jax.random.fold_in(jax.random.fold_in(stream_key, 6), position), (blocks,), jnp.float32, smallest / len(shards), largest / len(shards))
        loudness = loudness * jnp.repeat(jnp.exp(heights), shape[position] // blocks).reshape((-1,) + (1,) * (len(shape) - 1 - position))
    return loudness


def centred(stream_key, extent, scale, bound, cuts=(), held_as=jnp.bfloat16):
    loudness = block_scale(stream_key, extent, cuts, -0.22, 0.18) if cuts else 1.0
    result = jax.random.normal(stream_key, extent, jnp.float32) * scale * loudness
    return jnp.minimum(jnp.maximum(result, -bound), bound).astype(held_as)


def setup_inputs(seed: int = 0) -> dict:
    seeds = jax.random.split(jax.random.key(seed), 5)
    return {
        "key_states": centred(seeds[0], (PAIRS, 2, TOKENS, KVH * HD), 1.0, 6.0, ((2, 8), (3, 4))),
        "value_states": centred(seeds[1], (PAIRS, 2, TOKENS, KVH * HD), 1.0, 6.0, ((2, 8), (3, 4))),
        "bin_index": draw_bin_index(jax.random.fold_in(seeds[4], 71), 0),
        "retain_count": draw_retain_count(jax.random.fold_in(seeds[4], 71), 0),
    }


def similarity(states):
    first = states[0].astype(jnp.float32).reshape(TOKENS, KVH, HD)
    second = states[1].astype(jnp.float32).reshape(TOKENS, KVH, HD)
    inner_sum = lax.optimization_barrier(jnp.sum(first * second, axis=-1))
    first_sq = lax.optimization_barrier(jnp.sum(first * first, axis=-1))
    second_sq = lax.optimization_barrier(jnp.sum(second * second, axis=-1))
    return (inner_sum / jnp.sqrt((first_sq + 1.0) * (second_sq + 1.0))).T

def one_head(weight_pair, bins_row):
    summed = jax.ops.segment_sum(weight_pair.T, bins_row, num_segments=BINS)
    counted = jax.ops.segment_sum(jnp.ones_like(weight_pair[0]), bins_row, num_segments=BINS)
    return (summed.T, counted)

def reference(key_states, value_states, bin_index, retain_count):
    key_cos = lax.map(similarity, key_states)
    value_cos = lax.map(similarity, value_states)
    rounded = jnp.stack([key_cos, value_cos], axis=2).astype(jnp.bfloat16)
    rounded = lax.optimization_barrier(rounded)
    weights = rounded.astype(jnp.float32)
    histogram, counts = jax.vmap(jax.vmap(one_head))(weights, bin_index)
    pooled = lax.optimization_barrier(jnp.sum(counts, axis=1))
    cumulative = jnp.cumsum(jnp.cumsum(pooled, axis=0), axis=1)
    target = retain_count.astype(jnp.float32)[:, None]
    threshold = lax.optimization_barrier(jnp.sum((cumulative < target).astype(jnp.int32), axis=1)).astype(jnp.int32)
    return (histogram, threshold)
```

```python
import functools

import jax
import jax.numpy as jnp
from jax import lax
from jax.experimental import pallas as pl
from jax.experimental.pallas import tpu as pltpu
from jax.sharding import PartitionSpec as P

HD = 128
BINS = 4096
LANES = 128
VMEM = pltpu.MemorySpace.VMEM
NT = (((1,), (1,)), ((), ()))


def lane_onehot(row, lanes):
    return (lax.broadcasted_iota(jnp.int32, (lanes, row.shape[1]), 0) == (row & (lanes - 1))).astype(jnp.bfloat16)


def count_kernel(bin_ref, out_ref):
    pairs, heads, tokens = bin_ref.shape
    blocks = BINS // LANES
    high = lax.broadcasted_iota(jnp.int32, (blocks, tokens), 0)
    for p in range(pairs):
        total = None
        for h in range(heads):
            row = bin_ref[p, h : h + 1, :]
            left = (high == (row // LANES)).astype(jnp.bfloat16)
            part = lax.dot_general(left, lane_onehot(row, LANES), NT, preferred_element_type=jnp.float32)
            total = part if total is None else total + part
        out_ref[:, p] = total.reshape(2, blocks // 2, LANES)


def cosine(ref, h):
    first = ref[0, 0, :, h * HD : (h + 1) * HD].T.astype(jnp.float32)
    second = ref[0, 1, :, h * HD : (h + 1) * HD].T.astype(jnp.float32)
    inner = jnp.sum(first * second, axis=0, keepdims=True)
    first_sq = jnp.sum(first * first, axis=0, keepdims=True)
    second_sq = jnp.sum(second * second, axis=0, keepdims=True)
    return inner * lax.rsqrt((first_sq + 1.0) * (second_sq + 1.0))


def hist_kernel(ranges, key_ref, value_ref, bin_ref, out_ref):
    heads, tokens = bin_ref.shape[1:]
    lanes = out_ref.shape[-1]
    per = BINS // lanes // ranges
    rows = ranges * 2 * per
    index = lax.broadcasted_iota(jnp.int32, (rows, tokens), 0)
    high = (index // (2 * per)) * per + index % per
    is_key = (index // per) % 2 == 0
    for h in range(heads):
        row = bin_ref[0, h : h + 1, :]
        weight = jnp.where(is_key, cosine(key_ref, h), cosine(value_ref, h))
        left = jnp.where(high == (row // lanes), weight, 0.0).astype(jnp.bfloat16)
        table = lax.dot_general(left, lane_onehot(row, lanes), NT, preferred_element_type=jnp.float32)
        out_ref[:, 0, h] = table.reshape(ranges, 2 * per, lanes)


def threshold_kernel(own_ref, other_ref, mine_ref, target_ref, out_ref):
    pairs, blocks = own_ref.shape[0], BINS // LANES
    swap = mine_ref[0] == 1
    own, other = own_ref[...], other_ref[...]
    low = jnp.where(swap, other, own)
    top = jnp.where(swap, own, other)
    tables = []
    running = jnp.zeros((blocks, LANES), jnp.float32)
    for p in range(pairs):
        running = running + jnp.concatenate([low[p], top[p]], axis=0)
        tables.append(running)
    counts = jnp.concatenate(tables, axis=0)
    rows = pairs * blocks
    upper = (lax.broadcasted_iota(jnp.int32, (LANES, LANES), 0) <= lax.broadcasted_iota(jnp.int32, (LANES, LANES), 1)).astype(jnp.float32)
    within = jnp.dot(counts, upper, precision=lax.Precision.HIGHEST, preferred_element_type=jnp.float32)
    r = lax.broadcasted_iota(jnp.int32, (rows, rows), 0)
    c = lax.broadcasted_iota(jnp.int32, (rows, rows), 1)
    before = ((c < r) & (c // blocks == r // blocks)).astype(jnp.float32)
    ahead = jnp.dot(before, within, precision=lax.Precision.HIGHEST, preferred_element_type=jnp.float32)
    cumulative = within + ahead[:, LANES - 1 :]
    target = jnp.concatenate([jnp.full((blocks, LANES), target_ref[p].astype(jnp.float32)) for p in range(pairs)], axis=0)
    below = (cumulative < target).astype(jnp.bfloat16)
    sums = lax.dot_general(jnp.ones((8, LANES), jnp.bfloat16), below, NT, preferred_element_type=jnp.float32)
    group = (lax.broadcasted_iota(jnp.int32, (rows, LANES), 0) // blocks == lax.broadcasted_iota(jnp.int32, (rows, LANES), 1)).astype(jnp.bfloat16)
    found = jnp.dot(sums.astype(jnp.bfloat16), group, preferred_element_type=jnp.float32)
    out_ref[...] = found[0:1, 0:pairs].astype(jnp.int32)


def flip(axis_name, bit):
    return [(j, j ^ bit) for j in range(lax.axis_size(axis_name))]


def per_device(key_states, value_states, bin_index, retain_count):
    pairs, heads, tokens = bin_index.shape
    ranges = lax.axis_size("seq")
    lanes = min(LANES, BINS // ranges)
    per = BINS // lanes // ranges
    wide = heads * HD
    seq = lax.axis_index("seq")
    core = seq & 1

    counts = pl.pallas_call(
        count_kernel,
        out_shape=jax.ShapeDtypeStruct((2, pairs, BINS // LANES // 2, LANES), jnp.float32),
        in_specs=[pl.BlockSpec(memory_space=VMEM)],
        out_specs=pl.BlockSpec(memory_space=VMEM),
        compiler_params=pltpu.CompilerParams(vmem_limit_bytes=6 << 20),
        name="counts",
    )(bin_index)
    state_block = pl.BlockSpec((1, 2, tokens, wide), lambda p: (p, 0, 0, 0))
    hist = pl.pallas_call(
        functools.partial(hist_kernel, ranges),
        grid=(pairs,),
        out_shape=jax.ShapeDtypeStruct((ranges, pairs, heads, 2 * per, lanes), jnp.float32),
        in_specs=[state_block, state_block, pl.BlockSpec((1, heads, tokens), lambda p: (p, 0, 0))],
        out_specs=pl.BlockSpec((ranges, 1, heads, 2 * per, lanes), lambda p: (0, p, 0, 0, 0)),
        compiler_params=pltpu.CompilerParams(vmem_limit_bytes=12 << 20),
        name="hist",
    )(key_states, value_states, bin_index)

    pick = lambda x, k: lax.dynamic_index_in_dim(x, k, 0, keepdims=False)
    half = pick(counts, core) + lax.ppermute(pick(counts, 1 - core), "seq", flip("seq", 1))
    bit = 2
    while bit < ranges:
        half = half + lax.ppermute(half, "seq", flip("seq", bit))
        bit *= 2
    bit = 1
    while bit < lax.axis_size("tensor"):
        half = half + lax.ppermute(half, "tensor", flip("tensor", bit))
        bit *= 2
    other = lax.ppermute(half, "seq", flip("seq", 1))
    threshold = pl.pallas_call(
        threshold_kernel,
        out_shape=jax.ShapeDtypeStruct((1, pairs), jnp.int32),
        in_specs=[pl.BlockSpec(memory_space=VMEM)] * 2 + [pl.BlockSpec(memory_space=pltpu.MemorySpace.SMEM)] * 2,
        out_specs=pl.BlockSpec(memory_space=VMEM),
        compiler_params=pltpu.CompilerParams(vmem_limit_bytes=6 << 20),
        name="threshold",
    )(half, other, core.reshape(1), retain_count)

    tail = hist.shape[1:]
    bit = 1
    while bit < ranges:
        hist = hist.reshape(-1, 2, *tail)
        mine = lax.shift_right_logical(seq, bit.bit_length() - 1) & 1
        keep = lax.dynamic_index_in_dim(hist, mine, 1, keepdims=False)
        give = lax.dynamic_index_in_dim(hist, 1 - mine, 1, keepdims=False)
        hist = keep + lax.ppermute(give, "seq", flip("seq", bit))
        bit *= 2
    histogram = hist.reshape(pairs, heads, 2, per * lanes)
    return (histogram, threshold.reshape(pairs))


def solution(mesh):
    in_specs = (
        P(None, None, "seq", "tensor"),
        P(None, None, "seq", "tensor"),
        P(None, "tensor", "seq"),
        P(),
    )
    out_specs = (P(None, "tensor", None, "seq"), P())
    return jax.shard_map(
        per_device, mesh=mesh, in_specs=in_specs, out_specs=out_specs, check_vma=False
    )
```

```python
import functools

import jax
import jax.numpy as jnp
from jax import lax
from jax.experimental import pallas as pl
from jax.experimental.pallas import tpu as pltpu
from jax.sharding import PartitionSpec as P


HD = 128
BINS = 4096
LANES = 128
VMEM = pltpu.MemorySpace.VMEM
SMEM = pltpu.MemorySpace.SMEM
NT = (((1,), (1,)), ((), ()))
MIB = 1 << 20
PIECES = 2
HELD = (3, 2, 0)


def lane_onehot(row, lanes):
    return (lax.broadcasted_iota(jnp.int32, (lanes, row.shape[1]), 0) == (row & (lanes - 1))).astype(jnp.bfloat16)


def fetch(sources, targets, sems, first, count):
    return [
        [pltpu.make_async_copy(src.at[first + j], dst.at[j], sems.at[k, j]) for k, (src, dst) in enumerate(zip(sources, targets))]
        for j in range(count)
    ]


def start(copies):
    for pair in copies:
        for copy in pair:
            copy.start()


def count_kernel(ahead, key_ref, value_ref, bin_hbm, keep_ref, give_ref, bin_ref, key_next, value_next, sems, bin_sem):
    bin_copy = pltpu.make_async_copy(bin_hbm, bin_ref, bin_sem)
    bin_copy.start()
    copies = fetch((key_ref, value_ref), (key_next, value_next), sems, 0, ahead)
    start(copies)
    bin_copy.wait()
    pairs, heads, tokens = bin_ref.shape
    blocks = BINS // LANES
    rows = lax.broadcasted_iota(jnp.int32, (blocks, tokens), 0)
    high = rows ^ ((lax.axis_index("seq") & 1) * (blocks // 2))
    for p in range(pairs):
        total = None
        for h in range(heads):
            row = bin_ref[p, h : h + 1, :]
            left = (high == (row // LANES)).astype(jnp.bfloat16)
            part = lax.dot_general(left, lane_onehot(row, LANES), NT, preferred_element_type=jnp.float32)
            total = part if total is None else total + part
        keep_ref[p] = total[: blocks // 2]
        give_ref[p] = total[blocks // 2 :]
    for pair in copies:
        for copy in pair:
            copy.wait()


def cosine(ref, p, h):
    first = ref[p, 0, :, h * HD : (h + 1) * HD].T.astype(jnp.float32)
    second = ref[p, 1, :, h * HD : (h + 1) * HD].T.astype(jnp.float32)
    inner = jnp.sum(first * second, axis=0, keepdims=True)
    first_sq = jnp.sum(first * first, axis=0, keepdims=True)
    second_sq = jnp.sum(second * second, axis=0, keepdims=True)
    return inner * lax.rsqrt((first_sq + 1.0) * (second_sq + 1.0))


def hist_kernel(ranges, first, count, held, ahead, key_ref, value_ref, bin_ref, target_ref, key_held, value_held, *refs):
    if first:
        refs = refs[2:]
    keep_ref, give_ref = refs[:2]
    refs = refs[2:]
    states = (key_ref, value_ref)
    if ahead:
        goal_ref, key_next, value_next = refs[:3]
        refs = refs[3:]
    key_here, value_here, sems = refs[:3]
    here = fetch(states, (key_here, value_here), sems, first + held, count - held)
    start(here)
    later = []
    if ahead:
        later = fetch(states, (key_next, value_next), refs[3], first + count, ahead)
        start(later)
        target, target_sem = refs[4:]
        target_copy = pltpu.make_async_copy(target_ref, target, target_sem)
        target_copy.start()
    _, heads, tokens = bin_ref.shape
    lanes = keep_ref.shape[-1]
    per = BINS // lanes // ranges
    rows = ranges * 2 * per
    index = lax.broadcasted_iota(jnp.int32, (rows, tokens), 0)
    block = index // (2 * per)
    half = ranges // 2
    block = jnp.where(block < half, 2 * block, 2 * block - ranges + 1)
    high = (block ^ lax.axis_index("seq")) * per + index % per
    is_key = (index // per) % 2 == 0
    for j in range(count):
        keys, values, at = (key_held, value_held, j) if j < held else (key_here, value_here, j - held)
        if j >= held:
            for copy in here[at]:
                copy.wait()
        for h in range(heads):
            row = bin_ref[first + j, h : h + 1, :]
            weight = jnp.where(is_key, cosine(keys, at, h), cosine(values, at, h))
            left = jnp.where(high == (row // lanes), weight, 0.0).astype(jnp.bfloat16)
            table = lax.dot_general(left, lane_onehot(row, lanes), NT, preferred_element_type=jnp.float32)
            table = table.reshape(ranges, 2 * per, lanes)
            keep_ref[:, first + j, h] = table[:half]
            give_ref[:, first + j, h] = table[half:]
    for pair in later:
        for copy in pair:
            copy.wait()
    if ahead:
        target_copy.wait()
        goal_ref[...] = jnp.concatenate([jnp.full((1, LANES), target[p].astype(jnp.float32)) for p in range(goal_ref.shape[0])], axis=0)


def threshold_kernel(goal_ref, own_ref, other_ref, out_ref):
    pairs, half, lanes = own_ref.shape
    blocks = 2 * half
    swap = (lax.axis_index("seq") & 1) == 1
    own, other = own_ref[...], other_ref[...]
    low = jnp.where(swap, other, own)
    top = jnp.where(swap, own, other)
    counts = jnp.concatenate([low, top], axis=1).reshape(pairs * blocks, lanes)
    coarse = jnp.floor(counts * (1.0 / 256.0))
    fine = counts - coarse * 256.0
    column = lax.broadcasted_iota(jnp.int32, (lanes, 2 * lanes), 1)
    upper = ((lax.broadcasted_iota(jnp.int32, (lanes, 2 * lanes), 0) <= column) | (column >= lanes)).astype(jnp.bfloat16)
    sums = 256.0 * jnp.dot(coarse.astype(jnp.bfloat16), upper, preferred_element_type=jnp.float32)
    sums = sums + jnp.dot(fine.astype(jnp.bfloat16), upper, preferred_element_type=jnp.float32)
    within = sums[:, :lanes].reshape(pairs, blocks, lanes)
    total = sums[:, lanes:].reshape(pairs, blocks, lanes)
    line = lax.broadcasted_iota(jnp.int32, (blocks, lanes), 0)
    slot = lax.broadcasted_iota(jnp.int32, (pairs, lanes), 0)
    running = jnp.zeros((blocks, lanes), jnp.float32)
    found = jnp.zeros((pairs, lanes), jnp.float32)
    for p in range(pairs):
        upto = total[p]
        step = 1
        while step < blocks:
            upto = upto + jnp.where(line >= step, pltpu.roll(upto, step, 0), 0.0)
            step *= 2
        running = running + within[p] + (upto - total[p])
        below = (running < goal_ref[p : p + 1, :]).astype(jnp.float32)
        found = jnp.where(slot == p, jnp.sum(below, axis=0, keepdims=True), found)
    ones = jnp.ones((8, lanes), jnp.bfloat16)
    out_ref[...] = lax.dot_general(ones, found.astype(jnp.bfloat16), NT, preferred_element_type=jnp.float32)[0:1].astype(jnp.int32)


def final_kernel(*refs):
    *parts, out_ref = refs
    pairs, heads, rows, lanes = parts[-1].shape
    per = rows // 2
    for p in range(pairs):
        for h in range(heads):
            tile = parts[0][p, h]
            for part in parts[1:]:
                tile = tile + part[p, h]
            for r in range(2):
                for k in range(per):
                    out_ref[p, h, r : r + 1, k * lanes : (k + 1) * lanes] = tile[r * per + k : r * per + k + 1]


def per_device(key_states, value_states, bin_index, retain_count):
    pairs, heads, tokens = bin_index.shape
    ranges = lax.axis_size("seq")
    lanes = min(LANES, BINS // ranges)
    per = BINS // lanes // ranges
    wide = heads * HD
    states = [pltpu.with_memory_space_constraint(x, pltpu.HBM) for x in (key_states, value_states)]
    bins = pltpu.with_memory_space_constraint(bin_index, pltpu.HBM)
    target = pltpu.with_memory_space_constraint(retain_count, pltpu.HBM)
    whole = pl.BlockSpec(memory_space=VMEM)
    scalar = pl.BlockSpec(memory_space=SMEM)

    def permute(x, axis_name, bit):
        return lax.ppermute(x, axis_name, [(j, j ^ bit) for j in range(lax.axis_size(axis_name))])

    apart = pl.BlockSpec(memory_space=pl.ANY)
    states_of = lambda n: jax.ShapeDtypeStruct((n, 2, tokens, wide), key_states.dtype)
    scratch_of = lambda n: pltpu.VMEM((n, 2, tokens, wide), key_states.dtype)
    half = jax.ShapeDtypeStruct((pairs, BINS // LANES // 2, LANES), jnp.float32)
    mine, give, near_bins, *near = pl.pallas_call(
        functools.partial(count_kernel, HELD[0]),
        out_shape=(half, half, jax.ShapeDtypeStruct(bin_index.shape, jnp.int32), states_of(HELD[0]), states_of(HELD[0])),
        in_specs=[apart] * 3,
        out_specs=(whole,) * 5,
        scratch_shapes=[pltpu.SemaphoreType.DMA((2, HELD[0])), pltpu.SemaphoreType.DMA],
        compiler_params=pltpu.CompilerParams(vmem_limit_bytes=8 * MIB),
        name="counts",
    )(*states, bins)
    count = pairs // PIECES
    side = jax.ShapeDtypeStruct((ranges // 2, pairs, heads, 2 * per, lanes), jnp.float32)
    sides = ()
    for piece in range(PIECES):
        held, ahead = HELD[piece : piece + 2]
        extra = ahead and (jax.ShapeDtypeStruct((pairs, LANES), jnp.float32), states_of(ahead), states_of(ahead)) or ()
        sides = pl.pallas_call(
            functools.partial(hist_kernel, ranges, piece * count, count, held, ahead),
            out_shape=(side, side, *extra),
            in_specs=[apart, apart, whole, apart, whole, whole] + [apart] * len(sides),
            out_specs=(whole,) * (2 + len(extra)),
            scratch_shapes=[scratch_of(count - held)] * 2
            + [pltpu.SemaphoreType.DMA((2, count - held))]
            + [pltpu.SemaphoreType.DMA((2, ahead)), pltpu.SMEM((pairs,), jnp.int32), pltpu.SemaphoreType.DMA] * bool(ahead),
            input_output_aliases={6: 0, 7: 1} if sides else {},
            compiler_params=pltpu.CompilerParams(vmem_limit_bytes=14 * MIB),
            name="hist",
        )(*states, near_bins, target, *near, *sides)
        if extra:
            goal, near = sides[2], sides[3:]
            sides = sides[:2]
    keep, away = sides

    def plus(x, y):
        return x + y

    mine = plus(mine, permute(give, "seq", 1))
    bit = 2
    while bit < ranges:
        mine = plus(mine, permute(mine, "seq", bit))
        bit *= 2
    bit = 1
    while bit < lax.axis_size("tensor"):
        mine = plus(mine, permute(mine, "tensor", bit))
        bit *= 2
    other = permute(mine, "seq", 1)
    threshold = pl.pallas_call(
        threshold_kernel,
        out_shape=jax.ShapeDtypeStruct((1, pairs), jnp.int32),
        in_specs=[whole] * 3,
        out_specs=whole,
        compiler_params=pltpu.CompilerParams(vmem_limit_bytes=6 * MIB),
        name="threshold",
    )(goal, mine, other)

    got = permute(away, "seq", 1)
    parts = [[keep[j], got[j]] for j in range(ranges // 2)]
    total = lambda terms: functools.reduce(jnp.add, terms)
    bit = 2
    while bit < ranges:
        kept = []
        for j in range(0, len(parts), 2):
            part = permute(total(parts[j + 1]), "seq", bit)
            kept.append([*parts[j], part])
        parts = kept
        bit *= 2
    parts = parts[0]
    histogram = pl.pallas_call(
        final_kernel,
        out_shape=jax.ShapeDtypeStruct((pairs, heads, 2, per * lanes), jnp.float32),
        in_specs=[whole] * len(parts),
        out_specs=whole,
        compiler_params=pltpu.CompilerParams(vmem_limit_bytes=14 * MIB),
        name="final",
    )(*parts)
    return (histogram, threshold.reshape(pairs))


def solution(mesh):
    in_specs = (
        P(None, None, "seq", "tensor"),
        P(None, None, "seq", "tensor"),
        P(None, "tensor", "seq"),
        P(),
    )
    out_specs = (P(None, "tensor", None, "seq"), P())
    return jax.shard_map(per_device, mesh=mesh, in_specs=in_specs, out_specs=out_specs, check_vma=False)
```

```python
import functools

import jax
import jax.numpy as jnp
from jax import lax
from jax.experimental import pallas as pl
from jax.experimental.pallas import tpu as pltpu
from jax.sharding import PartitionSpec as P


HD = 128
BINS = 4096
LANES = 128
VMEM = pltpu.MemorySpace.VMEM
SMEM = pltpu.MemorySpace.SMEM
NT = (((1,), (1,)), ((), ()))
MIB = 1 << 20


def lane_onehot(row, lanes):
    return (lax.broadcasted_iota(jnp.int32, (lanes, row.shape[1]), 0) == (row & (lanes - 1))).astype(jnp.bfloat16)


def cosine(ref, p, h):
    first = ref[p, 0, :, h * HD : (h + 1) * HD].T.astype(jnp.float32)
    second = ref[p, 1, :, h * HD : (h + 1) * HD].T.astype(jnp.float32)
    inner = jnp.sum(first * second, axis=0, keepdims=True)
    first_sq = jnp.sum(first * first, axis=0, keepdims=True)
    second_sq = jnp.sum(second * second, axis=0, keepdims=True)
    return inner * lax.rsqrt((first_sq + 1.0) * (second_sq + 1.0))


def parity(x, size):
    odd = x
    for k in range(1, (size - 1).bit_length()):
        odd = odd ^ (x >> k)
    return odd & 1


def side_of_bins():
    return (lax.axis_index("seq") & 1) ^ parity(lax.axis_index("tensor"), lax.axis_size("tensor"))


def add_counts(bins, keep_ref, give_ref):
    pairs, heads, tokens = bins.shape
    blocks = BINS // LANES
    rows = lax.broadcasted_iota(jnp.int32, (blocks, tokens), 0)
    high = rows ^ (side_of_bins() * (blocks // 2))
    for p in range(pairs):
        total = None
        for h in range(heads):
            row = bins[p, h : h + 1, :]
            left = (high == (row // LANES)).astype(jnp.bfloat16)
            part = lax.dot_general(left, lane_onehot(row, LANES), NT, preferred_element_type=jnp.float32)
            total = part if total is None else total + part
        keep_ref[p] = total[: blocks // 2]
        give_ref[p] = total[blocks // 2 :]


def add_tables(ranges, bins, work, keys, values, keep_ref, give_ref):
    _, heads, tokens = bins.shape
    lanes = keep_ref.shape[-1]
    per = BINS // lanes // ranges
    rows = ranges * 2 * per
    index = lax.broadcasted_iota(jnp.int32, (rows, tokens), 0)
    block = index // (2 * per)
    half = ranges // 2
    away = (block >= half).astype(jnp.int32)
    block = block - half * away
    block = 2 * block + away
    high = (block ^ lax.axis_index("seq")) * per + index % per
    is_key = (index // per) % 2 == 0
    for p in work:
        for h in range(heads):
            row = bins[p, h : h + 1, :]
            weight = jnp.where(is_key, cosine(keys, p, h), cosine(values, p, h))
            left = jnp.where(high == (row // lanes), weight, 0.0).astype(jnp.bfloat16)
            table = lax.dot_general(left, lane_onehot(row, lanes), NT, preferred_element_type=jnp.float32)
            table = table.reshape(ranges, 2 * per, lanes)
            keep_ref[:, p, h] = table[:half]
            give_ref[:, p, h] = table[half:]


def count_kernel(bin_ref, target_ref, keep_ref, give_ref, bins, goal_ref, target, sem, target_sem):
    copy = pltpu.make_async_copy(bin_ref, bins, sem)
    target_copy = pltpu.make_async_copy(target_ref, target, target_sem)
    copy.start()
    target_copy.start()
    copy.wait()
    add_counts(bins, keep_ref, give_ref)
    target_copy.wait()
    goal_ref[...] = jnp.concatenate([jnp.full((1, LANES), target[p].astype(jnp.float32)) for p in range(goal_ref.shape[0])], axis=0)


def hist_kernel(ranges, work, key_ref, value_ref, bins, *refs):
    add_tables(ranges, bins, work, key_ref, value_ref, *refs[-2:])


def threshold_kernel(everything, goal_ref, own_ref, out_ref):
    pairs, blocks, lanes = own_ref.shape
    counts = own_ref[...].reshape(pairs * blocks, lanes)
    column = lax.broadcasted_iota(jnp.int32, (lanes, 2 * lanes), 1)
    upper = ((lax.broadcasted_iota(jnp.int32, (lanes, 2 * lanes), 0) <= column) | (column >= lanes)).astype(jnp.bfloat16)
    sums, scale, rest = 0.0, 1.0, counts
    while scale <= everything:
        above = jnp.floor(rest * (1.0 / 256.0))
        digit = rest - above * 256.0
        sums = sums + scale * jnp.dot(digit.astype(jnp.bfloat16), upper, preferred_element_type=jnp.float32)
        scale, rest = scale * 256.0, above
    within = sums[:, :lanes].reshape(pairs, blocks, lanes)
    total = sums[:, lanes:].reshape(pairs, blocks, lanes)
    line = lax.broadcasted_iota(jnp.int32, (blocks, lanes), 0)
    slot = lax.broadcasted_iota(jnp.int32, (pairs, lanes), 0)
    top_half = side_of_bins() == 1
    running = jnp.zeros((blocks, lanes), jnp.float32)
    found = jnp.zeros((pairs, lanes), jnp.float32)
    for p in range(pairs):
        upto = total[p]
        step = 1
        while step < blocks:
            upto = upto + jnp.where(line >= step, pltpu.roll(upto, step, 0), 0.0)
            step *= 2
        below_half = jnp.where(top_half, everything - upto[blocks - 1 :], 0.0)
        running = running + within[p] + (upto - total[p]) + below_half
        below = (running < goal_ref[p : p + 1, :]).astype(jnp.float32)
        found = jnp.where(slot == p, jnp.sum(below, axis=0, keepdims=True), found)
    out_ref[...] = found


def final_kernel(own_ref, other_ref, *refs):
    *parts, out_ref, threshold_ref = refs
    pairs, heads, rows, lanes = parts[-1].shape
    per = rows // 2
    for p in range(pairs):
        for h in range(heads):
            tile = parts[0][p, h]
            for part in parts[1:]:
                tile = tile + part[p, h]
            for r in range(2):
                for k in range(per):
                    out_ref[p, h, r : r + 1, k * lanes : (k + 1) * lanes] = tile[r * per + k : r * per + k + 1]
    found = (own_ref[...] + other_ref[...]).astype(jnp.bfloat16)
    ones = jnp.ones((8, found.shape[1]), jnp.bfloat16)
    threshold_ref[...] = lax.dot_general(ones, found, NT, preferred_element_type=jnp.float32)[0:1].astype(jnp.int32)


def per_device(key_states, value_states, bin_index, retain_count):
    pairs, heads, tokens = bin_index.shape
    ranges, columns = lax.axis_size("seq"), lax.axis_size("tensor")
    lanes = min(LANES, BINS // ranges)
    per = BINS // lanes // ranges
    bins = pltpu.with_memory_space_constraint(bin_index, pltpu.HBM)
    target = pltpu.with_memory_space_constraint(retain_count, pltpu.HBM)
    whole = pl.BlockSpec(memory_space=VMEM)
    scalar = pl.BlockSpec(memory_space=SMEM)

    def permute(x, tensor_bit, seq_bit):
        pairing = [(t * ranges + j, (t ^ tensor_bit) * ranges + (j ^ seq_bit)) for t in range(columns) for j in range(ranges)]
        return lax.ppermute(x, ("tensor", "seq"), pairing)

    apart = pl.BlockSpec(memory_space=pl.ANY)
    half = jax.ShapeDtypeStruct((pairs, BINS // LANES // 2, LANES), jnp.float32)
    side = jax.ShapeDtypeStruct((ranges // 2, pairs, heads, 2 * per, lanes), jnp.float32)
    mine, give, bins, goal = pl.pallas_call(
        count_kernel,
        out_shape=(half, half, jax.ShapeDtypeStruct(bin_index.shape, jnp.int32), jax.ShapeDtypeStruct((pairs, LANES), jnp.float32)),
        in_specs=[apart] * 2,
        out_specs=(whole,) * 4,
        scratch_shapes=[pltpu.SMEM((pairs,), jnp.int32), pltpu.SemaphoreType.DMA, pltpu.SemaphoreType.DMA],
        cost_estimate=pl.CostEstimate(flops=10000000000, bytes_accessed=100000000, transcendentals=0),
        compiler_params=pltpu.CompilerParams(vmem_limit_bytes=4 * MIB),
        name="counts",
    )(bins, target)
    sides = ()
    for piece in range(2):
        sides = pl.pallas_call(
            functools.partial(hist_kernel, ranges, range(pairs)[SPLIT[piece]]),
            out_shape=(side, side),
            in_specs=[whole] * 3 + [apart] * len(sides),
            out_specs=(whole,) * 2,
            input_output_aliases={3: 0, 4: 1} if sides else {},
            compiler_params=pltpu.CompilerParams(vmem_limit_bytes=16 * MIB),
            name="hist",
        )(key_states, value_states, bins, *sides)
    keep, away = sides

    def plus(x, y):
        return x + y

    mine = plus(mine, permute(give, 0, 1))
    bit = 2
    while bit < ranges:
        mine = plus(mine, permute(mine, 0, bit))
        bit *= 2
    bit = 1
    while bit < columns:
        mine = plus(mine, permute(mine, bit, 1))
        bit *= 2
    everything = float(tokens * ranges * heads * lax.axis_size("tensor"))
    found = pl.pallas_call(
        functools.partial(threshold_kernel, everything),
        out_shape=jax.ShapeDtypeStruct((pairs, LANES), jnp.float32),
        in_specs=[whole] * 2,
        out_specs=whole,
        compiler_params=pltpu.CompilerParams(vmem_limit_bytes=6 * MIB),
        name="threshold",
    )(goal, mine)
    other = permute(found, 0, 1)

    got = permute(away, 0, 1)
    parts = [[keep[j], got[j]] for j in range(ranges // 2)]
    total = lambda terms: functools.reduce(jnp.add, terms)
    bit = 2
    while bit < ranges:
        kept = []
        for j in range(0, len(parts), 2):
            part = permute(total(parts[j + 1]), 0, bit)
            kept.append([*parts[j], part])
        parts = kept
        bit *= 2
    parts = parts[0]
    histogram, threshold = pl.pallas_call(
        final_kernel,
        out_shape=(
            jax.ShapeDtypeStruct((pairs, heads, 2, per * lanes), jnp.float32),
            jax.ShapeDtypeStruct((1, pairs), jnp.int32),
        ),
        in_specs=[whole] * (2 + len(parts)),
        out_specs=(whole, whole),
        compiler_params=pltpu.CompilerParams(vmem_limit_bytes=14 * MIB),
        name="final",
    )(found, other, *parts)
    return (histogram, threshold.reshape(pairs))


SPLIT = (slice(0, 5), slice(5, None))


def solution(mesh):
    in_specs = (
        P(None, None, "seq", "tensor"),
        P(None, None, "seq", "tensor"),
        P(None, "tensor", "seq"),
        P(),
    )
    out_specs = (P(None, "tensor", None, "seq"), P())
    return jax.shard_map(per_device, mesh=mesh, in_specs=in_specs, out_specs=out_specs, check_vma=False)
```

```python
import functools

import jax
import jax.numpy as jnp
from jax import lax
from jax.experimental import pallas as pl
from jax.experimental.pallas import tpu as pltpu
from jax.sharding import PartitionSpec as P


HD = 128
BINS = 4096
LANES = 128
VMEM = pltpu.MemorySpace.VMEM
SMEM = pltpu.MemorySpace.SMEM
NT = (((1,), (1,)), ((), ()))
MIB = 1 << 20


def lane_onehot(row, lanes):
    return (lax.broadcasted_iota(jnp.int32, (lanes, row.shape[1]), 0) == (row & (lanes - 1))).astype(jnp.bfloat16)


def cosine(ref, p, h):
    first = ref[p, 0, :, h * HD : (h + 1) * HD].T.astype(jnp.float32)
    second = ref[p, 1, :, h * HD : (h + 1) * HD].T.astype(jnp.float32)
    inner = jnp.sum(first * second, axis=0, keepdims=True)
    first_sq = jnp.sum(first * first, axis=0, keepdims=True)
    second_sq = jnp.sum(second * second, axis=0, keepdims=True)
    return inner * lax.rsqrt((first_sq + 1.0) * (second_sq + 1.0))


def parity(x, size):
    odd = x
    for k in range(1, (size - 1).bit_length()):
        odd = odd ^ (x >> k)
    return odd & 1


def side_of_bins():
    return (lax.axis_index("seq") & 1) ^ parity(lax.axis_index("tensor"), lax.axis_size("tensor"))


def add_counts(bins, keep_ref, give_ref):
    pairs, heads, tokens = bins.shape
    blocks = BINS // LANES
    rows = lax.broadcasted_iota(jnp.int32, (blocks, tokens), 0)
    high = rows ^ (side_of_bins() * (blocks // 2))
    for p in range(pairs):
        total = None
        for h in range(heads):
            row = bins[p, h : h + 1, :]
            left = (high == (row // LANES)).astype(jnp.bfloat16)
            part = lax.dot_general(left, lane_onehot(row, LANES), NT, preferred_element_type=jnp.float32)
            total = part if total is None else total + part
        keep_ref[p] = total[: blocks // 2]
        give_ref[p] = total[blocks // 2 :]


def add_tables(ranges, bins, work, keys, values, keep_ref, give_ref):
    _, heads, tokens = bins.shape
    lanes = keep_ref.shape[-1]
    per = BINS // lanes // ranges
    rows = ranges * 2 * per
    index = lax.broadcasted_iota(jnp.int32, (rows, tokens), 0)
    block = index // (2 * per)
    half = ranges // 2
    away = (block >= half).astype(jnp.int32)
    block = block - half * away
    block = 2 * block + (parity(block, half) ^ away)
    high = (block ^ lax.axis_index("seq")) * per + index % per
    is_key = (index // per) % 2 == 0
    for p in work:
        for h in range(heads):
            row = bins[p, h : h + 1, :]
            weight = jnp.where(is_key, cosine(keys, p, h), cosine(values, p, h))
            left = jnp.where(high == (row // lanes), weight, 0.0).astype(jnp.bfloat16)
            table = lax.dot_general(left, lane_onehot(row, lanes), NT, preferred_element_type=jnp.float32)
            table = table.reshape(ranges, 2 * per, lanes)
            keep_ref[:, p, h] = table[:half]
            give_ref[:, p, h] = table[half:]


def count_kernel(bin_ref, target_ref, keep_ref, give_ref, bins, goal_ref, target, sem, target_sem):
    copy = pltpu.make_async_copy(bin_ref, bins, sem)
    target_copy = pltpu.make_async_copy(target_ref, target, target_sem)
    copy.start()
    target_copy.start()
    copy.wait()
    add_counts(bins, keep_ref, give_ref)
    target_copy.wait()
    goal_ref[...] = jnp.concatenate([jnp.full((1, LANES), target[p].astype(jnp.float32)) for p in range(goal_ref.shape[0])], axis=0)


def hist_kernel(ranges, work, key_ref, value_ref, bins, *refs):
    add_tables(ranges, bins, work, key_ref, value_ref, *refs[-2:])


def threshold_kernel(everything, goal_ref, own_ref, out_ref):
    pairs, blocks, lanes = own_ref.shape
    counts = own_ref[...].reshape(pairs * blocks, lanes)
    column = lax.broadcasted_iota(jnp.int32, (lanes, 2 * lanes), 1)
    upper = ((lax.broadcasted_iota(jnp.int32, (lanes, 2 * lanes), 0) <= column) | (column >= lanes)).astype(jnp.bfloat16)
    sums, scale, rest = 0.0, 1.0, counts
    while scale <= everything:
        above = jnp.floor(rest * (1.0 / 256.0))
        digit = rest - above * 256.0
        sums = sums + scale * jnp.dot(digit.astype(jnp.bfloat16), upper, preferred_element_type=jnp.float32)
        scale, rest = scale * 256.0, above
    within = sums[:, :lanes].reshape(pairs, blocks, lanes)
    total = sums[:, lanes:].reshape(pairs, blocks, lanes)
    line = lax.broadcasted_iota(jnp.int32, (blocks, lanes), 0)
    slot = lax.broadcasted_iota(jnp.int32, (pairs, lanes), 0)
    top_half = side_of_bins() == 1
    running = jnp.zeros((blocks, lanes), jnp.float32)
    found = jnp.zeros((pairs, lanes), jnp.float32)
    for p in range(pairs):
        upto = total[p]
        step = 1
        while step < blocks:
            upto = upto + jnp.where(line >= step, pltpu.roll(upto, step, 0), 0.0)
            step *= 2
        below_half = jnp.where(top_half, everything - upto[blocks - 1 :], 0.0)
        running = running + within[p] + (upto - total[p]) + below_half
        below = (running < goal_ref[p : p + 1, :]).astype(jnp.float32)
        found = jnp.where(slot == p, jnp.sum(below, axis=0, keepdims=True), found)
    out_ref[...] = found


def final_kernel(own_ref, other_ref, *refs):
    *parts, out_ref, threshold_ref = refs
    pairs, heads, rows, lanes = parts[-1].shape
    per = rows // 2
    for p in range(pairs):
        for h in range(heads):
            tile = parts[0][p, h]
            for part in parts[1:]:
                tile = tile + part[p, h]
            for r in range(2):
                for k in range(per):
                    out_ref[p, h, r : r + 1, k * lanes : (k + 1) * lanes] = tile[r * per + k : r * per + k + 1]
    found = (own_ref[...] + other_ref[...]).astype(jnp.bfloat16)
    ones = jnp.ones((8, found.shape[1]), jnp.bfloat16)
    threshold_ref[...] = lax.dot_general(ones, found, NT, preferred_element_type=jnp.float32)[0:1].astype(jnp.int32)


def per_device(key_states, value_states, bin_index, retain_count):
    pairs, heads, tokens = bin_index.shape
    ranges, columns = lax.axis_size("seq"), lax.axis_size("tensor")
    lanes = min(LANES, BINS // ranges)
    per = BINS // lanes // ranges
    bins = pltpu.with_memory_space_constraint(bin_index, pltpu.HBM)
    target = pltpu.with_memory_space_constraint(retain_count, pltpu.HBM)
    whole = pl.BlockSpec(memory_space=VMEM)
    scalar = pl.BlockSpec(memory_space=SMEM)

    def permute(x, tensor_bit, seq_bit):
        pairing = [(t * ranges + j, (t ^ tensor_bit) * ranges + (j ^ seq_bit)) for t in range(columns) for j in range(ranges)]
        return lax.ppermute(x, ("tensor", "seq"), pairing)

    apart = pl.BlockSpec(memory_space=pl.ANY)
    half = jax.ShapeDtypeStruct((pairs, BINS // LANES // 2, LANES), jnp.float32)
    side = jax.ShapeDtypeStruct((ranges // 2, pairs, heads, 2 * per, lanes), jnp.float32)
    mine, give, bins, goal = pl.pallas_call(
        count_kernel,
        out_shape=(half, half, jax.ShapeDtypeStruct(bin_index.shape, jnp.int32), jax.ShapeDtypeStruct((pairs, LANES), jnp.float32)),
        in_specs=[apart] * 2,
        out_specs=(whole,) * 4,
        scratch_shapes=[pltpu.SMEM((pairs,), jnp.int32), pltpu.SemaphoreType.DMA, pltpu.SemaphoreType.DMA],
        cost_estimate=pl.CostEstimate(flops=10000000000, bytes_accessed=100000000, transcendentals=0),
        compiler_params=pltpu.CompilerParams(vmem_limit_bytes=4 * MIB),
        name="counts",
    )(bins, target)
    sides = ()
    for piece in range(2):
        sides = pl.pallas_call(
            functools.partial(hist_kernel, ranges, range(pairs)[SPLIT[piece]]),
            out_shape=(side, side),
            in_specs=[whole] * 3 + [apart] * len(sides),
            out_specs=(whole,) * 2,
            input_output_aliases={3: 0, 4: 1} if sides else {},
            compiler_params=pltpu.CompilerParams(vmem_limit_bytes=16 * MIB),
            name="hist",
        )(key_states, value_states, bins, *sides)
    keep, away = sides

    def plus(x, y):
        return x + y

    mine = plus(mine, permute(give, 0, 1))
    bit = 2
    while bit < ranges:
        mine = plus(mine, permute(mine, 0, bit))
        bit *= 2
    mine = functools.reduce(jnp.add, [mine] + [permute(mine, k, k.bit_count() & 1) for k in range(1, columns)])
    everything = float(tokens * ranges * heads * lax.axis_size("tensor"))
    found = pl.pallas_call(
        functools.partial(threshold_kernel, everything),
        out_shape=jax.ShapeDtypeStruct((pairs, LANES), jnp.float32),
        in_specs=[whole] * 2,
        out_specs=whole,
        compiler_params=pltpu.CompilerParams(vmem_limit_bytes=6 * MIB),
        name="threshold",
    )(goal, mine)
    other = permute(found, 0, 1)

    got = permute(away, 0, 1)
    parts = [[keep[j], got[j]] for j in range(ranges // 2)]
    total = lambda terms: functools.reduce(jnp.add, terms)
    bit = 2
    while bit < ranges:
        kept = []
        for j in range(0, len(parts), 2):
            part = permute(total(parts[j + 1]), 0, bit | 1)
            kept.append([*parts[j], part])
        parts = kept
        bit *= 2
    parts = parts[0]
    histogram, threshold = pl.pallas_call(
        final_kernel,
        out_shape=(
            jax.ShapeDtypeStruct((pairs, heads, 2, per * lanes), jnp.float32),
            jax.ShapeDtypeStruct((1, pairs), jnp.int32),
        ),
        in_specs=[whole] * (2 + len(parts)),
        out_specs=(whole, whole),
        compiler_params=pltpu.CompilerParams(vmem_limit_bytes=14 * MIB),
        name="final",
    )(found, other, *parts)
    return (histogram, threshold.reshape(pairs))


SPLIT = (slice(0, 5), slice(5, None))


def solution(mesh):
    in_specs = (
        P(None, None, "seq", "tensor"),
        P(None, None, "seq", "tensor"),
        P(None, "tensor", "seq"),
        P(),
    )
    out_specs = (P(None, "tensor", None, "seq"), P())
    return jax.shard_map(per_device, mesh=mesh, in_specs=in_specs, out_specs=out_specs, check_vma=False)
```
